32 devices in a mesh: tm: 4 (over y, x), space: 8 (over z, core).
Axes of the slice: x: 2, y: 2, z: 4, core: 2. Of those that a mesh axis runs over, the one named last changes fastest.
Arguments:
- hidden_in: bfloat16 [8, 16, 32, 5120], P('tm', 'space'), may hold values from -6 to 6
- queries: bfloat16 [8, 16, 32, 5120], P('tm', 'space'), may hold values from -250 to 250
- keys: bfloat16 [8, 16, 32, 5120], P('tm', 'space'), may hold values from -250 to 250
- values: bfloat16 [8, 16, 32, 5120], P('tm', 'space'), may hold values from -6 to 6
- query_gain: float32 [5120], replicated, may hold values from 0.5 to 3
- key_gain: float32 [5120], replicated, may hold values from 0.5 to 3
- reach_time: int32 [40], replicated, may hold values from 0 to 1
- reach_rows: int32 [40], replicated, may hold values from 0 to 1
- reach_cols: int32 [40], replicated, may hold values from 0 to 2
- out_weight: bfloat16 [5120, 5120], P('space', 'tm'), may hold values from -0.25 to 0.25
- gate: float32 [5120], replicated, may hold values from -1.5 to 1.5
Outputs:
- output: bfloat16 [8, 16, 32, 5120], P('tm', 'space')
The draws below stay inside these ranges and needn't reach their ends.
All inputs are finite; a program needn't handle non-finite values.
Results may differ from the reference program's by a relative error of at most 0.013.
The reference program's roundings to bfloat16 on the way (of `query_norm`, `key_norm`, `rounded` and `attention`) count: a program that leaves them out, or rounds other values in their place, can miss the bound.
Values may be sent and summed in bfloat16 or wider, within the bound.
A program may use at most 128 MiB of HBM per device.

```python
import math
import jax
import jax.numpy as jnp
from jax import lax

D = 5120
HEADS = 40
FR = 2
RH = 2
NW = 32
TW = 8
INNER = 5120
NF = 8
NH = 16


def lifted_field(key, salt):
    base = jax.random.normal(jax.random.fold_in(key, salt), (NF, NH, NW, INNER), jnp.float32)
    return jnp.clip(base, -6.0, 6.0)


def draw_queries(key, part):
    field = lifted_field(key, 11)
    return jnp.clip(field, -250.0, 250.0).astype(jnp.bfloat16)


def draw_keys(key, part):
    field = lifted_field(key, 21)
    return jnp.clip(field, -250.0, 250.0).astype(jnp.bfloat16)


def plant(result, own_key, least, largest):
    longest = result.shape.index(max(result.shape))
    spots = []
    for shift in (0, 1):
        where = [jax.random.randint(jax.random.fold_in(own_key, axis), (), 0, length) for axis, length in enumerate(result.shape)]
        where[longest] = (where[longest] + shift) % result.shape[longest]
        spots.append(tuple(where))
    return result.at[spots[0]].set(least).at[spots[1]].set(largest)


def shard_levels(rng, shape, shards, low, top_value):
    loudness = 1.0
    for position, shards_of in shards:
        steps = jax.random.uniform(jax.random.fold_in(jax.random.fold_in(rng, 6), position), (shards_of,), jnp.float32, low / len(shards), top_value / len(shards))
        loudness = loudness * jnp.repeat(jnp.exp(steps), shape[position] // shards_of).reshape((-1,) + (1,) * (len(shape) - 1 - position))
    return loudness


def gaussian(rng, shape, scale, limit, split=(), held_as=jnp.bfloat16):
    result = scale * jax.random.normal(rng, shape, jnp.float32)
    if split:
        result = result * shard_levels(rng, shape, split, -0.22, 0.18)
    return jnp.clip(result, -limit, limit).astype(held_as)


def setup_inputs(seed: int = 0) -> dict:
    key_list = jax.random.split(jax.random.key(seed), 12)
    hidden_in = gaussian(key_list[0], (NF, NH, NW, D), 1.0, 6.0, ((0, 4), (1, 8)))
    queries = draw_queries(jax.random.fold_in(key_list[11], 71), 0)
    keys = draw_keys(jax.random.fold_in(key_list[11], 71), 0)
    values = gaussian(key_list[3], (NF, NH, NW, INNER), 1.0, 6.0, ((0, 4), (1, 8)))
    query_gain = jnp.clip(jnp.exp(jax.random.uniform(key_list[4], (INNER,), jnp.float32, math.log(0.5), math.log(3.0))), 0.5, 3.0)
    key_gain = jnp.clip(jnp.exp(jax.random.uniform(key_list[5], (INNER,), jnp.float32, math.log(0.5), math.log(3.0))), 0.5, 3.0)
    reach_time = plant(jax.random.randint(key_list[6], (HEADS,), 0, 2), jax.random.fold_in(key_list[6], 1), 0, 1).astype(jnp.int32)
    reach_rows = plant(jax.random.randint(key_list[7], (HEADS,), 0, 2), jax.random.fold_in(key_list[7], 1), 0, 1).astype(jnp.int32)
    reach_cols = plant(jax.random.randint(key_list[8], (HEADS,), 0, 3), jax.random.fold_in(key_list[8], 1), 0, 2).astype(jnp.int32)
    out_weight = gaussian(key_list[9], (INNER, D), (INNER // 8) ** -0.5, 0.25, ((0, 8), (1, 4)))
    gate = jnp.clip(jax.random.uniform(key_list[10], (D,), jnp.float32, -1.5, 1.5), -1.5, 1.5)
    return dict(hidden_in=hidden_in, queries=queries, keys=keys, values=values, query_gain=query_gain, key_gain=key_gain, reach_time=reach_time, reach_rows=reach_rows, reach_cols=reach_cols, out_weight=out_weight, gate=gate)


def normalize(source, gain):
    values_f = source.astype(jnp.float32)
    mean_square = lax.optimization_barrier(jnp.mean(values_f * values_f, axis=-1, keepdims=True))
    return (values_f * lax.rsqrt(mean_square + 1e-06) * gain).astype(jnp.bfloat16)

def attend(query_block, key_region, value_region, first_frame, first_row, frame_count, row_count, reach_time, reach_rows, reach_cols):
    frames_here, rows_here, columns, inner = query_block.shape
    head_count = reach_time.shape[0]
    head_width = inner // head_count
    query_flat = query_block.reshape(-1, head_count, head_width).astype(jnp.float32)
    key_flat = key_region.reshape(-1, head_count, head_width).astype(jnp.float32)
    value_flat = value_region.reshape(-1, head_count, head_width).astype(jnp.float32)
    frame_q = first_frame + jnp.arange(frames_here, dtype=jnp.int32)
    frame_k = first_frame - 1 + jnp.arange(frames_here + 2, dtype=jnp.int32)
    row_q = first_row + jnp.arange(rows_here, dtype=jnp.int32)
    row_k = first_row - 1 + jnp.arange(rows_here + 2, dtype=jnp.int32)
    tiles = jnp.arange(columns, dtype=jnp.int32) // TW
    query_shape = (frames_here, rows_here, columns)
    key_shape = (frames_here + 2, rows_here + 2, columns)
    query_frame = jnp.broadcast_to(frame_q[:, None, None], query_shape).reshape(-1)
    query_row = jnp.broadcast_to(row_q[None, :, None], query_shape).reshape(-1)
    query_tile = jnp.broadcast_to(tiles[None, None, :], query_shape).reshape(-1)
    key_frame = jnp.broadcast_to(frame_k[:, None, None], key_shape).reshape(-1)
    key_row = jnp.broadcast_to(row_k[None, :, None], key_shape).reshape(-1)
    key_tile = jnp.broadcast_to(tiles[None, None, :], key_shape).reshape(-1)
    frame_gap = jnp.abs(query_frame[:, None] - key_frame[None, :])
    row_gap = jnp.abs(query_row[:, None] - key_row[None, :])
    tile_gap = jnp.abs(query_tile[:, None] - key_tile[None, :])
    inside = (key_frame >= 0) & (key_frame < frame_count) & (key_row >= 0) & (key_row < row_count)
    allowed = (frame_gap[None] <= reach_time[:, None, None]) & (row_gap[None] <= reach_rows[:, None, None])
    allowed = allowed & (tile_gap[None] <= reach_cols[:, None, None]) & inside[None, None, :]
    scores = jnp.einsum('qhd,khd->hqk', query_flat, key_flat) * head_width ** (-0.5)
    masked = jnp.where(allowed, scores, -jnp.inf)
    row_peak = lax.optimization_barrier(jnp.max(masked, axis=2, keepdims=True))
    weights = jnp.exp(masked - row_peak)
    totals = lax.optimization_barrier(jnp.sum(weights, axis=2, keepdims=True))
    rounded = weights.astype(jnp.bfloat16)
    mixed = jnp.einsum('hqk,khd->qhd', rounded.astype(jnp.float32), value_flat)
    mixed = mixed / jnp.transpose(totals, (1, 0, 2))
    return mixed.reshape(mixed.shape[0], inner).astype(jnp.bfloat16)

def reference(hidden_in, queries, keys, values, query_gain, key_gain, reach_time, reach_rows, reach_cols, out_weight, gate):
    query_norm = normalize(queries, query_gain)
    key_norm = normalize(keys, key_gain)
    padding = ((1, 1), (1, 1), (0, 0), (0, 0))
    key_pad = jnp.pad(key_norm, padding)
    value_pad = jnp.pad(values, padding)
    row_blocks = NH // RH
    block_count = NF // FR * row_blocks

    def one_block(block_index):
        first_frame = (block_index // row_blocks * FR).astype(jnp.int32)
        first_row = (block_index % row_blocks * RH).astype(jnp.int32)
        anchor = jnp.zeros((), jnp.int32)
        query_block = lax.dynamic_slice(query_norm, (first_frame, first_row, anchor, anchor), (FR, RH, NW, INNER))
        key_region = lax.dynamic_slice(key_pad, (first_frame, first_row, anchor, anchor), (FR + 2, RH + 2, NW, INNER))
        value_region = lax.dynamic_slice(value_pad, (first_frame, first_row, anchor, anchor), (FR + 2, RH + 2, NW, INNER))
        attention = attend(query_block, key_region, value_region, first_frame, first_row, NF, NH, reach_time, reach_rows, reach_cols)
        hidden_block = lax.dynamic_slice(hidden_in, (first_frame, first_row, anchor, anchor), (FR, RH, NW, D))
        hidden_flat = hidden_block.reshape(-1, D).astype(jnp.float32)
        branch = jnp.dot(attention, out_weight, preferred_element_type=jnp.float32)
        return (hidden_flat + gate * branch).astype(jnp.bfloat16).reshape(FR, RH, NW, D)
    blocks = lax.map(one_block, jnp.arange(block_count, dtype=jnp.int32))
    blocks = blocks.reshape(NF // FR, NH // RH, FR, RH, NW, D)
    return jnp.transpose(blocks, (0, 2, 1, 3, 4, 5)).reshape(NF, NH, NW, D)
```

```python
import jax
import jax.numpy as jnp
from jax import lax
from jax.sharding import PartitionSpec as P

TW = 8


def passed_along(block, axis, distance):
    devices = range(lax.axis_size(axis))
    route = [(i - distance, i) for i in devices if i - distance in devices]
    return lax.ppermute(block, axis, route)


def normalize(source, gain):
    values_f = source.astype(jnp.float32)
    mean_square = jnp.mean(values_f * values_f, axis=-1, keepdims=True)
    return (values_f * lax.rsqrt(mean_square + 1e-06) * gain).astype(jnp.bfloat16)


def attend(
    query_block,
    key_region,
    value_region,
    first_frame,
    first_row,
    frame_count,
    row_count,
    reach_time,
    reach_rows,
    reach_cols,
):
    frames_here, rows_here, columns, inner = query_block.shape
    head_count = reach_time.shape[0]
    head_width = inner // head_count
    query_flat = query_block.reshape(-1, head_count, head_width)
    key_flat = key_region.reshape(-1, head_count, head_width)
    value_flat = value_region.reshape(-1, head_count, head_width)
    frame_q = first_frame + jnp.arange(frames_here, dtype=jnp.int32)
    frame_k = first_frame - 1 + jnp.arange(frames_here + 2, dtype=jnp.int32)
    row_q = first_row + jnp.arange(rows_here, dtype=jnp.int32)
    row_k = first_row - 1 + jnp.arange(rows_here + 2, dtype=jnp.int32)
    tiles = jnp.arange(columns, dtype=jnp.int32) // TW
    query_shape = (frames_here, rows_here, columns)
    key_shape = (frames_here + 2, rows_here + 2, columns)
    query_frame = jnp.broadcast_to(frame_q[:, None, None], query_shape).reshape(-1)
    query_row = jnp.broadcast_to(row_q[None, :, None], query_shape).reshape(-1)
    query_tile = jnp.broadcast_to(tiles[None, None, :], query_shape).reshape(-1)
    key_frame = jnp.broadcast_to(frame_k[:, None, None], key_shape).reshape(-1)
    key_row = jnp.broadcast_to(row_k[None, :, None], key_shape).reshape(-1)
    key_tile = jnp.broadcast_to(tiles[None, None, :], key_shape).reshape(-1)
    frame_gap = jnp.abs(query_frame[:, None] - key_frame[None, :])
    row_gap = jnp.abs(query_row[:, None] - key_row[None, :])
    tile_gap = jnp.abs(query_tile[:, None] - key_tile[None, :])
    inside = (key_frame >= 0) & (key_frame < frame_count) & (key_row >= 0) & (key_row < row_count)
    allowed = (frame_gap[None] <= reach_time[:, None, None]) & (
        row_gap[None] <= reach_rows[:, None, None]
    )
    allowed = allowed & (tile_gap[None] <= reach_cols[:, None, None]) & inside[None, None, :]
    scores = jnp.einsum(
        "qhd,khd->hqk", query_flat, key_flat, preferred_element_type=jnp.float32
    ) * head_width ** (-0.5)
    masked = jnp.where(allowed, scores, -jnp.inf)
    row_peak = jnp.max(masked, axis=2, keepdims=True)
    weights = jnp.exp(masked - row_peak)
    totals = jnp.sum(weights, axis=2, keepdims=True)
    rounded = weights.astype(jnp.bfloat16)
    mixed = jnp.einsum("hqk,khd->qhd", rounded, value_flat, preferred_element_type=jnp.float32)
    mixed = mixed / jnp.transpose(totals, (1, 0, 2))
    return mixed.reshape(mixed.shape[0], inner).astype(jnp.bfloat16)


def shards(
    hidden_in,
    queries,
    keys,
    values,
    query_gain,
    key_gain,
    reach_time,
    reach_rows,
    reach_cols,
    out_weight,
    gate,
):
    frames_here, rows_here, columns, inner = queries.shape
    width = hidden_in.shape[3]
    query_norm = normalize(queries, query_gain)
    key_norm = normalize(keys, key_gain)
    stacked = jnp.stack([key_norm, values])
    below_frame = passed_along(stacked[:, -1:], "tm", 1)
    above_frame = passed_along(stacked[:, :1], "tm", -1)
    below_own = passed_along(stacked[:, :, -1:], "space", 1)
    above_own = passed_along(stacked[:, :, :1], "space", -1)
    margins = jnp.concatenate([below_frame, above_frame], axis=1)
    below_margin = passed_along(margins[:, :, -1:], "space", 1)
    above_margin = passed_along(margins[:, :, :1], "space", -1)
    framed = jnp.concatenate([below_frame, stacked, above_frame], axis=1)
    below_rows = jnp.concatenate([below_margin[:, :1], below_own, below_margin[:, 1:]], axis=1)
    above_rows = jnp.concatenate([above_margin[:, :1], above_own, above_margin[:, 1:]], axis=1)
    region = jnp.concatenate([below_rows, framed, above_rows], axis=2)
    first_frame = lax.axis_index("tm") * frames_here
    first_row = lax.axis_index("space") * rows_here
    frame_count = frames_here * lax.axis_size("tm")
    row_count = rows_here * lax.axis_size("space")
    attention = attend(
        query_norm,
        region[0],
        region[1],
        first_frame,
        first_row,
        frame_count,
        row_count,
        reach_time,
        reach_rows,
        reach_cols,
    )
    token_count = attention.shape[0]
    gathered_rows = lax.all_gather(out_weight, "space", axis=0, tiled=True)
    attention, gathered_rows = lax.optimization_barrier((attention, gathered_rows))
    group_terms = jnp.dot(
        lax.all_gather(attention, "tm", axis=0, tiled=True),
        gathered_rows,
        preferred_element_type=jnp.float32,
    ).astype(jnp.bfloat16)
    branch = lax.all_to_all(group_terms, "tm", split_axis=0, concat_axis=1, tiled=True)
    residual = hidden_in.reshape(token_count, width).astype(jnp.float32)
    output = (residual + gate * branch.astype(jnp.float32)).astype(jnp.bfloat16)
    return output.reshape(frames_here, rows_here, columns, width)


def solution(mesh):
    in_specs = (
        P("tm", "space", None, None),
        P("tm", "space", None, None),
        P("tm", "space", None, None),
        P("tm", "space", None, None),
        P(),
        P(),
        P(),
        P(),
        P(),
        P("space", "tm"),
        P(),
    )
    out_specs = P("tm", "space", None, None)
    return jax.shard_map(shards, mesh=mesh, in_specs=in_specs, out_specs=out_specs, check_vma=False)
```

```python
import functools
import math

import jax
import jax.numpy as jnp
from jax import lax
from jax.experimental import pallas as pl
from jax.experimental.pallas import tpu as pltpu
from jax.sharding import PartitionSpec as P

TW = 8
REACHES = [(a, b, c) for a in range(2) for b in range(2) for c in range(3)]


def normalize(source, gain):
    values_f = source.astype(jnp.float32)
    mean_square = jnp.mean(values_f * values_f, axis=-1, keepdims=True)
    return (values_f * lax.rsqrt(mean_square + 1e-06) * gain).astype(jnp.bfloat16)


def mask_table(frames_here, rows_here, columns, first_frame, first_row, frame_count, row_count):
    query_shape = (frames_here, rows_here, columns)
    key_shape = (frames_here + 2, rows_here + 2, columns)

    def spread(vector, axis, shape):
        dims = [1, 1, 1]
        dims[axis] = vector.shape[0]
        return jnp.broadcast_to(vector.reshape(dims), shape).reshape(-1)

    tiles = jnp.arange(columns, dtype=jnp.int32) // TW
    query_parts = (
        spread(first_frame + jnp.arange(frames_here, dtype=jnp.int32), 0, query_shape),
        spread(first_row + jnp.arange(rows_here, dtype=jnp.int32), 1, query_shape),
        spread(tiles, 2, query_shape),
    )
    key_parts = (
        spread(first_frame - 1 + jnp.arange(frames_here + 2, dtype=jnp.int32), 0, key_shape),
        spread(first_row - 1 + jnp.arange(rows_here + 2, dtype=jnp.int32), 1, key_shape),
        spread(tiles, 2, key_shape),
    )
    inside = (
        (key_parts[0] >= 0)
        & (key_parts[0] < frame_count)
        & (key_parts[1] >= 0)
        & (key_parts[1] < row_count)
    )
    gaps = [jnp.abs(q[:, None] - k[None, :]) for q, k in zip(query_parts, key_parts)]
    reach = jnp.array(REACHES, jnp.int32)
    allowed = inside[None, None, :]
    for axis in range(3):
        allowed = allowed & (gaps[axis][None] <= reach[:, axis][:, None, None])
    return jnp.where(allowed, 0.0, -1e30).astype(jnp.float32)


def kernel(
    heads,
    group,
    kind_ref,
    query_ref,
    mask_ref,
    hidden_ref,
    gate_ref,
    kv_ref,
    weight_ref,
    out_ref,
    region,
    weights,
    mixed,
    total,
    outgoing,
    incoming,
    local_sem,
    halo_send,
    halo_recv,
    near_send,
    pair_send,
    weight_recv,
    mixed_send,
    mixed_recv,
    back_send,
    back_recv,
):
    t = lax.axis_index("tm")
    s = lax.axis_index("space")
    nt = lax.axis_size("tm")
    ns = lax.axis_size("space")
    chips = ns // 2
    frames, rows, columns, inner = kv_ref.shape[1:]
    tokens = frames * rows * columns
    keys_here = (frames + 2) * (rows + 2) * columns
    width = inner // heads
    depth, cols = weight_ref.shape

    def remote(source, target, send, recv, tm, space):
        return pltpu.make_async_remote_copy(
            src_ref=source,
            dst_ref=target,
            send_sem=send,
            recv_sem=recv,
            device_id=(tm, space),
            device_id_type=pl.DeviceIdType.MESH,
        )

    has_low_t, has_high_t = t > 0, t < nt - 1
    has_low_s, has_high_s = s > 0, s < ns - 1
    own_f, own_r = pl.ds(1, frames), pl.ds(1, rows)

    def halo(i, source, target, tm, space):
        return remote(source, target, halo_send.at[i], halo_recv.at[i], tm, space)

    up_f = halo(0, kv_ref.at[:, frames - 1], region.at[:, 0, own_r], t + 1, s)
    down_f = halo(1, kv_ref.at[:, 0], region.at[:, frames + 1, own_r], t - 1, s)
    up_r = halo(2, kv_ref.at[:, :, rows - 1], region.at[:, own_f, 0], t, s + 1)
    down_r = halo(3, kv_ref.at[:, :, 0], region.at[:, own_f, rows + 1], t, s - 1)
    corners = []
    for i, (frame, has_frame) in enumerate(((0, has_low_t), (frames + 1, has_high_t))):
        corners.append((
            halo(4 + 2 * i, region.at[:, frame, rows], region.at[:, frame, 0], t, s + 1),
            has_frame & has_high_s, has_frame & has_low_s,
        ))
        corners.append((
            halo(5 + 2 * i, region.at[:, frame, 1], region.at[:, frame, rows + 1], t, s - 1),
            has_frame & has_low_s, has_frame & has_high_s,
        ))
    straight = [
        (up_f, has_high_t, has_low_t),
        (down_f, has_low_t, has_high_t),
        (up_r, has_high_s, has_low_s),
        (down_r, has_low_s, has_high_s),
    ]

    def block(ref, b):
        return ref.at[pl.ds(pl.multiple_of(b * depth, depth), depth)]

    partner = s + 1 - 2 * lax.rem(s, 2)

    def near(k, b, way, first):
        space = s + 2 if way == 0 else s - 2
        source = weight_ref if first else block(weights, b)
        return remote(source, block(weights, b), near_send.at[way, k], weight_recv.at[b], t, space)

    def pair(k, b, way, first):
        source = weight_ref if first else block(weights, b)
        return remote(source, block(weights, b), pair_send.at[way, k], weight_recv.at[b], t, partner)

    def arrived(b):
        remote(block(weights, b), block(weights, b), pair_send.at[0, 0], weight_recv.at[b], t, partner).wait_recv()

    for copy, sends, _ in straight:
        pl.when(sends)(copy.start)
    pl.when(s + 2 < ns)(near(0, s, 0, True).start)
    pl.when(s >= 2)(near(0, s, 1, True).start)
    pair(0, s, 0, True).start()
    own_kv = pltpu.make_async_copy(kv_ref, region.at[:, own_f, own_r], local_sem.at[0])
    own_kv.start()
    own_weight = pltpu.make_async_copy(weight_ref, block(weights, s), local_sem.at[1])
    own_weight.start()

    def clear_frame(frame):
        def run():
            for part in range(2):
                for row in range(rows + 2):
                    region[part, frame, row] = jnp.zeros((columns, inner), jnp.bfloat16)
        return run

    def clear_row(row):
        def run():
            for part in range(2):
                for frame in range(frames + 2):
                    region[part, frame, row] = jnp.zeros((columns, inner), jnp.bfloat16)
        return run

    pl.when(jnp.logical_not(has_low_t))(clear_frame(0))
    pl.when(jnp.logical_not(has_high_t))(clear_frame(frames + 1))
    pl.when(jnp.logical_not(has_low_s))(clear_row(0))
    pl.when(jnp.logical_not(has_high_s))(clear_row(rows + 1))

    def relay(k):
        low, high = s - 2 * k, s + 2 * k

        @pl.when(low >= 0)
        def _():
            arrived(low)
            pl.when(s + 2 < ns)(near(k, low, 0, False).start)
            pair(k, low, 0, False).start()

        @pl.when(high < ns)
        def _():
            arrived(high)
            pl.when(s >= 2)(near(k, high, 1, False).start)
            pair(k, high, 1, False).start()

    for copy, _, receives in straight[:2]:
        pl.when(receives)(copy.wait_recv)
    for copy, sends, _ in corners:
        pl.when(sends)(copy.start)
    relay(1)
    for copy, _, receives in straight[2:]:
        pl.when(receives)(copy.wait_recv)
    for copy, _, receives in corners:
        pl.when(receives)(copy.wait_recv)
    own_kv.wait()

    groups = heads // group
    span = group * width

    def gather(g, d):
        at = (t, slice(None), pl.ds(pl.multiple_of(g * span, span), span))
        return remote(
            mixed.at[at], mixed.at[at], mixed_send.at[d - 1, g], mixed_recv.at[t, g],
            lax.rem(t + d, nt), s,
        )

    def one_group(g, carry):
        for i in range(group):
            h = g * group + i
            lanes = pl.ds(pl.multiple_of(h * width, width), width)
            query = query_ref[:, lanes]
            key = region[0, :, :, :, lanes].reshape(keys_here, width)
            value = region[1, :, :, :, lanes].reshape(keys_here, width)
            scores = lax.dot_general(
                query, key, (((1,), (1,)), ((), ())), preferred_element_type=jnp.float32
            ) * width ** (-0.5)
            scores = scores + mask_ref[kind_ref[h]]
            part = jnp.exp(scores - jnp.max(scores, axis=1, keepdims=True))
            sums = jnp.sum(part, axis=1, keepdims=True)
            result = jnp.dot(part.astype(jnp.bfloat16), value, preferred_element_type=jnp.float32)
            mixed[t, :, lanes] = (result / sums).astype(jnp.bfloat16)
        for d in range(1, nt):
            gather(g, d).start()
        return carry

    lax.fori_loop(0, groups, one_group, 0)

    def gathered(g, carry):
        for d in range(1, nt):
            other = lax.rem(t + d, nt)
            at = (other, slice(None), pl.ds(pl.multiple_of(g * span, span), span))
            remote(mixed.at[at], mixed.at[at], mixed_send.at[d - 1, g], mixed_recv.at[other, g], t, s).wait_recv()
        return carry

    chip_depth = 2 * depth
    piece = chip_depth * 128 // math.gcd(chip_depth, 128)
    tile = 256 if cols % 256 == 0 else 128

    def multiply(start, first):
        feature = pl.ds(pl.multiple_of(start, piece), piece)

        def column(j, carry):
            lanes = pl.ds(pl.multiple_of(j * tile, tile), tile)
            left = mixed[:, :, feature].reshape(nt * tokens, piece)
            product = jnp.dot(left, weights[feature, lanes], preferred_element_type=jnp.float32)
            if first:
                total[:, lanes] = product
            else:
                total[:, lanes] += product
            return carry

        lax.fori_loop(0, cols // tile, column, 0)

    chip = s // 2
    half = lax.rem(s, 2)

    def partner_arrived(c):
        arrived(2 * c + 1 - half)

    if piece == chip_depth:
        for k in range(2, chips - 1):
            relay(k)
        lax.fori_loop(0, groups, gathered, 0)
        own_weight.wait()
        partner_arrived(chip)
        multiply(chip * piece, True)

        def add(k):
            for other in (chip - k, chip + k):
                @pl.when((other >= 0) & (other < chips))
                def _():
                    partner_arrived(other)
                    multiply(other * piece, False)

        for k in range(1, chips - 1):
            add(k)
        if chips > 2:
            relay(chips - 1)
        if chips > 1:
            add(chips - 1)
    else:
        for k in range(2, chips):
            relay(k)
        lax.fori_loop(0, groups, gathered, 0)
        own_weight.wait()

        def all_arrived(c, carry):
            partner_arrived(c)
            return carry

        lax.fori_loop(0, chips, all_arrived, 0)
        multiply(0, True)

        def add_piece(p, carry):
            multiply(p * piece, False)
            return carry

        lax.fori_loop(1, inner // piece, add_piece, 0)

    def back(d):
        other = lax.rem(t + d, nt)
        return remote(outgoing.at[d - 1], incoming.at[d - 1], back_send.at[d - 1], back_recv.at[d - 1], other, s)

    def own_rows(owner):
        return pl.ds(pl.multiple_of(owner * tokens, tokens), tokens)

    for d in range(1, nt):
        outgoing[d - 1] = total[own_rows(lax.rem(t + d, nt)), :].astype(jnp.bfloat16)
        back(d).start()

    def finish(owner, branch):
        lanes = pl.ds(pl.multiple_of(owner * cols, cols), cols)
        out_ref[:, lanes] = (
            hidden_ref[:, lanes].astype(jnp.float32) + gate_ref[:, lanes] * branch
        ).astype(jnp.bfloat16)

    finish(t, total[own_rows(t), :])
    for d in range(1, nt):
        back(d).wait_recv()
        finish(lax.rem(t + nt - d, nt), incoming[d - 1].astype(jnp.float32))

    for copy, sends, _ in straight + corners:
        pl.when(sends)(copy.wait_send)
    for k in range(chips):
        low, high = s - 2 * k, s + 2 * k
        pl.when((low >= 0) & (s + 2 < ns))(near(k, low, 0, k == 0).wait_send)
        pl.when((high < ns) & (s >= 2))(near(k, high, 1, k == 0).wait_send)
        pl.when(low >= 0)(pair(k, low, 0, k == 0).wait_send)
        if k > 0:
            pl.when(high < ns)(pair(k, high, 1, False).wait_send)

    def sent(g, carry):
        for d in range(1, nt):
            gather(g, d).wait_send()
        return carry

    lax.fori_loop(0, groups, sent, 0)
    for d in range(1, nt):
        back(d).wait_send()


def shards(
    hidden_in,
    queries,
    keys,
    values,
    query_gain,
    key_gain,
    reach_time,
    reach_rows,
    reach_cols,
    out_weight,
    gate,
):
    frames, rows, columns, inner = queries.shape
    width = hidden_in.shape[3]
    heads = reach_time.shape[0]
    tokens = frames * rows * columns
    nt, ns = lax.axis_size("tm"), lax.axis_size("space")
    depth, cols = out_weight.shape
    query_norm = normalize(queries, query_gain).reshape(tokens, inner)
    stacked = jnp.stack([normalize(keys, key_gain), values])
    masks = mask_table(
        frames, rows, columns,
        lax.axis_index("tm") * frames, lax.axis_index("space") * rows,
        frames * nt, rows * ns,
    )
    kind = reach_time * 6 + reach_rows * 3 + reach_cols
    group = 5 if heads % 5 == 0 else 1
    vmem = pl.BlockSpec(memory_space=pltpu.VMEM)
    hbm = pl.BlockSpec(memory_space=pl.ANY)
    dma = pltpu.SemaphoreType.DMA
    output = pl.pallas_call(
        functools.partial(kernel, heads, group),
        out_shape=jax.ShapeDtypeStruct((tokens, width), jnp.bfloat16),
        in_specs=[pl.BlockSpec(memory_space=pltpu.SMEM), vmem, vmem, vmem, vmem, hbm, hbm],
        out_specs=vmem,
        scratch_shapes=[
            pltpu.VMEM((2, frames + 2, rows + 2, columns, inner), jnp.bfloat16),
            pltpu.VMEM((depth * ns, cols), jnp.bfloat16),
            pltpu.VMEM((nt, tokens, inner), jnp.bfloat16),
            pltpu.VMEM((nt * tokens, cols), jnp.float32),
            pltpu.VMEM((nt - 1, tokens, cols), jnp.bfloat16),
            pltpu.VMEM((nt - 1, tokens, cols), jnp.bfloat16),
            dma((2,)),
            dma((8,)),
            dma((8,)),
            dma((2, ns // 2)),
            dma((2, ns // 2)),
            dma((ns,)),
            dma((nt - 1, heads // group)),
            dma((nt, heads // group)),
            dma((nt - 1,)),
            dma((nt - 1,)),
        ],
        compiler_params=pltpu.CompilerParams(
            has_side_effects=True, vmem_limit_bytes=60 * 1024 * 1024
        ),
    )(
        kind,
        query_norm,
        masks,
        hidden_in.reshape(tokens, width),
        gate.reshape(1, width),
        stacked,
        out_weight,
    )
    return output.reshape(frames, rows, columns, width)


def solution(mesh):
    in_specs = (
        P("tm", "space", None, None),
        P("tm", "space", None, None),
        P("tm", "space", None, None),
        P("tm", "space", None, None),
        P(),
        P(),
        P(),
        P(),
        P(),
        P("space", "tm"),
        P(),
    )
    out_specs = P("tm", "space", None, None)
    return jax.shard_map(shards, mesh=mesh, in_specs=in_specs, out_specs=out_specs, check_vma=False)
```

```python
import functools
import math

import jax
import jax.numpy as jnp
import numpy as np
from jax import lax
from jax.experimental import pallas as pl
from jax.experimental.pallas import tpu as pltpu
from jax.sharding import PartitionSpec as P

TW = 8
REACHES = [(a, b, c) for a in range(2) for b in range(2) for c in range(3)]


def normalized(source, gain):
    values_f = source.astype(jnp.float32)
    mean_square = jnp.mean(values_f * values_f, axis=-1, keepdims=True)
    return (values_f * lax.rsqrt(mean_square + 1e-06) * gain).astype(jnp.bfloat16)


def places(frames, rows, columns, margin):
    grid = np.meshgrid(
        np.arange(-margin, frames + margin),
        np.arange(-margin, rows + margin),
        np.arange(columns) // TW,
        indexing="ij",
    )
    return np.stack([axis.reshape(-1) for axis in grid]).astype(np.int32)


def kernel(
    heads,
    group,
    time_ref,
    rows_ref,
    cols_ref,
    raw_query_ref,
    key_ref,
    query_gain_ref,
    key_gain_ref,
    query_place_ref,
    key_place_ref,
    gate_ref,
    value_ref,
    weight_ref,
    hidden_in_ref,
    out_ref,
    query_ref,
    mask_ref,
    hidden_ref,
    region,
    weights,
    mixed,
    total,
    outgoing,
    incoming,
    local_sem,
    own_sem,
    halo_send,
    halo_recv,
    near_send,
    pair_send,
    weight_recv,
    mixed_send,
    mixed_recv,
    back_send,
    back_recv,
):
    t = lax.axis_index("tm")
    s = lax.axis_index("space")
    nt = lax.axis_size("tm")
    ns = lax.axis_size("space")
    chips = ns // 2
    frames, rows, columns, inner = value_ref.shape
    tokens = frames * rows * columns
    keys_here = (frames + 2) * (rows + 2) * columns
    width = inner // heads
    depth, cols = weight_ref.shape

    def remote(source, target, send, recv, tm, space):
        return pltpu.make_async_remote_copy(
            src_ref=source,
            dst_ref=target,
            send_sem=send,
            recv_sem=recv,
            device_id=(tm, space),
            device_id_type=pl.DeviceIdType.MESH,
        )

    has_low_t, has_high_t = t > 0, t < nt - 1
    has_low_s, has_high_s = s > 0, s < ns - 1
    own_f, own_r = pl.ds(1, frames), pl.ds(1, rows)

    def halo(i, source, target, tm, space):
        return remote(source, target, halo_send.at[i], halo_recv.at[i], tm, space)

    straight = []
    for part, whole in ((1, value_ref), (0, region.at[0, own_f, own_r])):
        straight += [
            (halo(4 * part, whole.at[frames - 1], region.at[part, 0, own_r], t + 1, s), has_high_t, has_low_t),
            (halo(4 * part + 1, whole.at[0], region.at[part, frames + 1, own_r], t - 1, s), has_low_t, has_high_t),
            (halo(4 * part + 2, whole.at[:, rows - 1], region.at[part, own_f, 0], t, s + 1), has_high_s, has_low_s),
            (halo(4 * part + 3, whole.at[:, 0], region.at[part, own_f, rows + 1], t, s - 1), has_low_s, has_high_s),
        ]
    corners = []
    for i, (frame, has_frame) in enumerate(((0, has_low_t), (frames + 1, has_high_t))):
        corners.append((
            halo(8 + 2 * i, region.at[:, frame, rows], region.at[:, frame, 0], t, s + 1),
            has_frame & has_high_s, has_frame & has_low_s,
        ))
        corners.append((
            halo(9 + 2 * i, region.at[:, frame, 1], region.at[:, frame, rows + 1], t, s - 1),
            has_frame & has_low_s, has_frame & has_high_s,
        ))
    parts, lane = weights.shape[0], weights.shape[2]

    def block(b, p):
        return weights.at[p, pl.ds(pl.multiple_of(b * depth, depth), depth)]

    def own_block(p):
        return weight_ref.at[:, pl.ds(pl.multiple_of(p * lane, lane), lane)]

    partner = s + 1 - 2 * lax.rem(s, 2)

    def near(k, b, way, p, first):
        space = s + 2 if way == 0 else s - 2
        source = own_block(p) if first else block(b, p)
        return remote(source, block(b, p), near_send.at[way, k, p], weight_recv.at[b, p], t, space)

    def pair(k, b, way, p, first):
        source = own_block(p) if first else block(b, p)
        return remote(source, block(b, p), pair_send.at[way, k, p], weight_recv.at[b, p], t, partner)

    def arrived(b, p):
        remote(block(b, p), block(b, p), pair_send.at[0, 0, p], weight_recv.at[b, p], t, partner).wait_recv()

    def each_part(low, high, run):
        def body(p, carry):
            run(p)
            return carry

        lax.fori_loop(low, high, body, 0)

    for copy, sends, _ in straight[:4]:
        pl.when(sends)(copy.start)

    def first_part(p):
        pl.when(s + 2 < ns)(near(0, s, 0, p, True).start)
        pl.when(s >= 2)(near(0, s, 1, p, True).start)
        pair(0, s, 0, p, True).start()
        pltpu.make_async_copy(own_block(p), block(s, p), own_sem.at[p]).start()

    each_part(0, parts, first_part)
    own_value = pltpu.make_async_copy(value_ref, region.at[1, own_f, own_r], local_sem.at[0])
    own_value.start()
    own_hidden = pltpu.make_async_copy(hidden_in_ref, hidden_ref, local_sem.at[1])
    own_hidden.start()

    step = 16 if columns % 16 == 0 else columns
    for frame in range(frames):
        for row in range(rows):
            for column in range(0, columns, step):
                at = slice(column, column + step)
                region[0, 1 + frame, 1 + row, at] = normalized(key_ref[frame, row, at], key_gain_ref[...])

    def query_rows(i, carry):
        at = pl.ds(pl.multiple_of(i * 16, 16), 16)
        query_ref[at] = normalized(raw_query_ref[at], query_gain_ref[...])
        return carry

    lax.fori_loop(0, tokens // 16, query_rows, 0)
    for copy, sends, _ in straight[4:]:
        pl.when(sends)(copy.start)

    def clear_frame(frame):
        def run():
            for part in range(2):
                for row in range(rows + 2):
                    region[part, frame, row] = jnp.zeros((columns, inner), jnp.bfloat16)
        return run

    def clear_row(row):
        def run():
            for part in range(2):
                for frame in range(frames + 2):
                    region[part, frame, row] = jnp.zeros((columns, inner), jnp.bfloat16)
        return run

    pl.when(jnp.logical_not(has_low_t))(clear_frame(0))
    pl.when(jnp.logical_not(has_high_t))(clear_frame(frames + 1))
    pl.when(jnp.logical_not(has_low_s))(clear_row(0))
    pl.when(jnp.logical_not(has_high_s))(clear_row(rows + 1))

    frame_k, row_k, tile_k = key_place_ref[0:1], key_place_ref[1:2], key_place_ref[2:3]
    inside = (frame_k >= -t * frames) & (frame_k < (nt - t) * frames)
    inside = inside & (row_k >= -s * rows) & (row_k < (ns - s) * rows)
    outside = jnp.where(inside, 0, 9)
    frame_gap = jnp.abs(query_place_ref[:, 0:1] - frame_k) + outside
    row_gap = jnp.abs(query_place_ref[:, 1:2] - row_k)
    tile_gap = jnp.abs(query_place_ref[:, 2:3] - tile_k)
    for i, (reach_t, reach_r, reach_c) in enumerate(REACHES):
        allowed = (frame_gap <= reach_t) & (row_gap <= reach_r) & (tile_gap <= reach_c)
        mask_ref[i] = jnp.where(allowed, 0.0, -1e30)

    def relay(k, p):
        low, high = s - 2 * k, s + 2 * k

        @pl.when(low >= 0)
        def _():
            arrived(low, p)
            pl.when(s + 2 < ns)(near(k, low, 0, p, False).start)
            pair(k, low, 0, p, False).start()

        @pl.when(high < ns)
        def _():
            arrived(high, p)
            pl.when(s >= 2)(near(k, high, 1, p, False).start)
            pair(k, high, 1, p, False).start()

    def relay_parts(k, low, high):
        if 1 <= k < chips:
            each_part(low, high, functools.partial(relay, k))

    early = parts // 2
    last = chips - 1
    if last > 1:
        relay_parts(1, 0, early)
    for copy, _, receives in straight[0:2] + straight[4:6]:
        pl.when(receives)(copy.wait_recv)
    for copy, sends, _ in corners:
        pl.when(sends)(copy.start)
    for copy, _, receives in straight[2:4] + straight[6:8]:
        pl.when(receives)(copy.wait_recv)
    for copy, _, receives in corners:
        pl.when(receives)(copy.wait_recv)
    if last > 1:
        relay_parts(1, early, parts)
    own_value.wait()

    groups = heads // group
    span = group * width

    def gather(g, d):
        at = (t, slice(None), pl.ds(pl.multiple_of(g * span, span), span))
        return remote(
            mixed.at[at], mixed.at[at], mixed_send.at[d - 1, g], mixed_recv.at[t, g],
            lax.rem(t + d, nt), s,
        )

    def one_group(g, carry):
        for i in range(group):
            h = g * group + i
            lanes = pl.ds(pl.multiple_of(h * width, width), width)
            query = query_ref[:, lanes]
            key = region[0, :, :, :, lanes].reshape(keys_here, width)
            value = region[1, :, :, :, lanes].reshape(keys_here, width)
            scores = lax.dot_general(
                query, key, (((1,), (1,)), ((), ())), preferred_element_type=jnp.float32
            ) * width ** (-0.5)
            scores = scores + mask_ref[time_ref[h] * 6 + rows_ref[h] * 3 + cols_ref[h]]
            part = jnp.exp(scores - jnp.max(scores, axis=1, keepdims=True))
            sums = jnp.sum(part, axis=1, keepdims=True)
            result = jnp.dot(part.astype(jnp.bfloat16), value, preferred_element_type=jnp.float32)
            mixed[t, :, lanes] = (result / sums).astype(jnp.bfloat16)
        for d in range(1, nt):
            gather(g, d).start()
        return carry

    ahead = groups * 5 // 8
    lax.fori_loop(0, ahead, one_group, 0)
    if last > 2:
        relay_parts(2, 0, parts)
    lax.fori_loop(ahead, groups, one_group, 0)
    for k in range(3, last):
        relay_parts(k, 0, parts)

    def gathered(g, carry):
        for d in range(1, nt):
            other = lax.rem(t + d, nt)
            at = (other, slice(None), pl.ds(pl.multiple_of(g * span, span), span))
            remote(mixed.at[at], mixed.at[at], mixed_send.at[d - 1, g], mixed_recv.at[other, g], t, s).wait_recv()
        return carry

    chip_depth = 2 * depth
    piece = chip_depth * 128 // math.gcd(chip_depth, 128)

    def multiply(start, p, first):
        feature = pl.ds(pl.multiple_of(start, piece), piece)
        left = mixed[:, :, feature].reshape(nt * tokens, piece)
        product = jnp.dot(left, weights[p, feature], preferred_element_type=jnp.float32)
        if first:
            total[p] = product
        else:
            total[p] += product

    chip = s // 2
    half = lax.rem(s, 2)

    def add(k, p):
        for other in (chip - k, chip + k):
            @pl.when((other >= 0) & (other < chips))
            def _():
                arrived(2 * other + 1 - half, p)
                multiply(other * piece, p, False)

    def own_rows(owner):
        return pl.ds(pl.multiple_of(owner * tokens, tokens), tokens)

    def back(d, p):
        other = lax.rem(t + d, nt)
        return remote(
            outgoing.at[d - 1, p], incoming.at[d - 1, p], back_send.at[d - 1, p], back_recv.at[d - 1, p], other, s
        )

    def send_back(p):
        for d in range(1, nt):
            outgoing[d - 1, p] = total[p, own_rows(lax.rem(t + d, nt)), :].astype(jnp.bfloat16)
            back(d, p).start()

    def own_part(p):
        pltpu.make_async_copy(own_block(p), block(s, p), own_sem.at[p]).wait()
        arrived(partner, p)

    lax.fori_loop(0, groups, gathered, 0)
    if piece == chip_depth:
        def begin(p):
            own_part(p)
            multiply(chip * piece, p, True)
            for k in range(1, last):
                add(k, p)

        each_part(0, parts, begin)

        def conclude(p):
            if last > 0:
                relay(last, p)
                add(last, p)
            send_back(p)

        each_part(0, parts, conclude)
    else:
        def conclude(p):
            own_part(p)
            if last > 0:
                relay(last, p)
            for k in range(1, chips):
                for other in (chip - k, chip + k):
                    @pl.when((other >= 0) & (other < chips))
                    def _():
                        arrived(2 * other + 1 - half, p)
            multiply(0, p, True)

            def add_piece(i, carry):
                multiply(i * piece, p, False)
                return carry

            lax.fori_loop(1, inner // piece, add_piece, 0)
            send_back(p)

        each_part(0, parts, conclude)

    own_hidden.wait()

    def finish(owner, p, branch):
        lanes = pl.ds(pl.multiple_of(owner * cols + p * lane, lane), lane)
        out_ref[:, lanes] = (
            hidden_ref[:, lanes].astype(jnp.float32) + gate_ref[:, lanes] * branch
        ).astype(jnp.bfloat16)

    def finish_own(p):
        finish(t, p, total[p, own_rows(t), :])

    def finish_others(p):
        for d in range(1, nt):
            back(d, p).wait_recv()
            finish(lax.rem(t + nt - d, nt), p, incoming[d - 1, p].astype(jnp.float32))

    each_part(0, parts, finish_own)
    each_part(0, parts, finish_others)

    for copy, sends, _ in straight + corners:
        pl.when(sends)(copy.wait_send)
    for k in range(chips):
        low, high = s - 2 * k, s + 2 * k

        def weight_sent(p):
            pl.when((low >= 0) & (s + 2 < ns))(near(k, low, 0, p, k == 0).wait_send)
            pl.when((high < ns) & (s >= 2))(near(k, high, 1, p, k == 0).wait_send)
            pl.when(low >= 0)(pair(k, low, 0, p, k == 0).wait_send)
            if k > 0:
                pl.when(high < ns)(pair(k, high, 1, p, False).wait_send)

        each_part(0, parts, weight_sent)

    def sent(g, carry):
        for d in range(1, nt):
            gather(g, d).wait_send()
        return carry

    lax.fori_loop(0, groups, sent, 0)

    def back_sent(p):
        for d in range(1, nt):
            back(d, p).wait_send()

    each_part(0, parts, back_sent)


def shards(
    hidden_in,
    queries,
    keys,
    values,
    query_gain,
    key_gain,
    reach_time,
    reach_rows,
    reach_cols,
    out_weight,
    gate,
):
    frames, rows, columns, inner = queries.shape
    width = hidden_in.shape[3]
    heads = reach_time.shape[0]
    tokens = frames * rows * columns
    nt, ns = lax.axis_size("tm"), lax.axis_size("space")
    depth, cols = out_weight.shape
    group = 5 if heads % 5 == 0 else 1
    vmem = pl.BlockSpec(memory_space=pltpu.VMEM)
    hbm = pl.BlockSpec(memory_space=pl.ANY)
    dma = pltpu.SemaphoreType.DMA
    lane = 256 if cols % 256 == 0 else 128
    parts = cols // lane
    output = pl.pallas_call(
        functools.partial(kernel, heads, group),
        out_shape=jax.ShapeDtypeStruct((tokens, width), jnp.bfloat16),
        in_specs=[pl.BlockSpec(memory_space=pltpu.SMEM)] * 3 + [vmem] * 7 + [hbm] * 3,
        out_specs=vmem,
        scratch_shapes=[
            pltpu.VMEM((tokens, inner), jnp.bfloat16),
            pltpu.VMEM((len(REACHES), tokens, (frames + 2) * (rows + 2) * columns), jnp.float32),
            pltpu.VMEM((tokens, width), jnp.bfloat16),
            pltpu.VMEM((2, frames + 2, rows + 2, columns, inner), jnp.bfloat16),
            pltpu.VMEM((parts, depth * ns, lane), jnp.bfloat16),
            pltpu.VMEM((nt, tokens, inner), jnp.bfloat16),
            pltpu.VMEM((parts, nt * tokens, lane), jnp.float32),
            pltpu.VMEM((nt - 1, parts, tokens, lane), jnp.bfloat16),
            pltpu.VMEM((nt - 1, parts, tokens, lane), jnp.bfloat16),
            dma((2,)),
            dma((parts,)),
            dma((12,)),
            dma((12,)),
            dma((2, ns // 2, parts)),
            dma((2, ns // 2, parts)),
            dma((ns, parts)),
            dma((nt - 1, heads // group)),
            dma((nt, heads // group)),
            dma((nt - 1, parts)),
            dma((nt - 1, parts)),
        ],
        compiler_params=pltpu.CompilerParams(
            has_side_effects=True, vmem_limit_bytes=60 * 1024 * 1024
        ),
    )(
        reach_time,
        reach_rows,
        reach_cols,
        queries.reshape(tokens, inner),
        keys,
        query_gain.reshape(1, inner),
        key_gain.reshape(1, inner),
        places(frames, rows, columns, 0).T,
        places(frames, rows, columns, 1),
        gate.reshape(1, width),
        values,
        out_weight,
        hidden_in.reshape(tokens, width),
    )
    return output.reshape(frames, rows, columns, width)


def solution(mesh):
    in_specs = (
        P("tm", "space", None, None),
        P("tm", "space", None, None),
        P("tm", "space", None, None),
        P("tm", "space", None, None),
        P(),
        P(),
        P(),
        P(),
        P(),
        P("space", "tm"),
        P(),
    )
    out_specs = P("tm", "space", None, None)
    return jax.shard_map(shards, mesh=mesh, in_specs=in_specs, out_specs=out_specs, check_vma=False)
```
